32 devices in a mesh: mom: 4 (over y, core), tm: 4 (over z), pt: 2 (over x).
Axes of the slice: x: 2, y: 2, z: 4, core: 2. Of those that a mesh axis runs over, the one named last changes fastest.
Arguments:
- chi_time: bfloat16 [16, 8, 896, 896], P('tm', 'mom', 'pt'), may hold values from -4 to 4
- green: bfloat16 [8, 16, 896, 896], P('mom', 'tm', 'pt'), may hold values from -6 to 6
- band_coeffs: bfloat16 [896, 1024], replicated, may hold values from -1 to 1
Outputs:
- self_energy: float32 [8, 16, 1024], P('mom', 'tm', 'pt')
The draws below stay inside these ranges and needn't reach their ends.
All inputs are finite; a program needn't handle non-finite values.
Results may differ from the reference program's by a relative error of at most 0.009.
Values may be sent and summed in bfloat16 or wider, within the bound.
A program may use at most 128 MiB of HBM per device.

```python
import math
import jax
import jax.numpy as jnp
from jax import lax

NK = 8
NT = 16
NP = 896
NB = 1024
ORDER = 8


def draw_chi_time(key, part):
    shape = (NT, NK, NP, NP)
    values = jnp.clip(jax.random.normal(key, shape, jnp.float32), -4.0, 4.0)
    return values.astype(jnp.bfloat16)


def block_scale(key, extent, cuts, low, largest):
    level, own = 1.0, jax.random.fold_in(key, 6)
    for position, parts in cuts:
        draws = jnp.exp(jax.random.uniform(jax.random.fold_in(own, position), (parts,), jnp.float32, low / len(cuts), largest / len(cuts)))
        level = level * jnp.repeat(draws, extent[position] // parts).reshape([-1 if axis == position else 1 for axis in range(len(extent))])
    return level


def bell_draw(key, shape, deviation, bound, pieces=(), kind=jnp.bfloat16):
    entries = deviation * jax.random.normal(key, shape, jnp.float32)
    if pieces:
        entries = entries * block_scale(key, shape, pieces, -0.22, 0.18)
    return jnp.clip(entries, -bound, bound).astype(kind)


def setup_inputs(seed: int = 0) -> dict:
    keys = jax.random.split(jax.random.key(seed), 4)
    return {
        "chi_time": draw_chi_time(jax.random.fold_in(keys[3], 71), 0),
        "green": bell_draw(keys[1], (NK, NT, NP, NP), 1.0, 6.0, ((0, 4), (1, 4), (2, 2))),
        "band_coeffs": bell_draw(keys[2], (NP, NB), 28 ** -0.5, 1.0),
    }


COUPLING = 0.8

def cosine_table(count):
    index = jnp.arange(count, dtype=jnp.float32) + 0.5
    angle = jnp.pi * index[:, None] * index[None, :] / count
    return (jnp.sqrt(jnp.float32(2.0 / count)) * jnp.cos(angle)).astype(jnp.bfloat16)

def hartley_table(count):
    index = jnp.arange(count, dtype=jnp.float32)
    angle = 2.0 * jnp.pi * index[:, None] * index[None, :] / count
    return (jnp.cos(angle) + jnp.sin(angle)) / jnp.sqrt(jnp.float32(count))

def series_tile(tile):
    power = tile
    total = tile.astype(jnp.float32)
    for term in range(ORDER - 1):
        power = jnp.dot(power, tile, preferred_element_type=jnp.float32).astype(jnp.bfloat16)
        total = total + power.astype(jnp.float32)
    return total.astype(jnp.bfloat16)

def reference(chi_time, green, band_coeffs):
    highest = lax.Precision.HIGHEST
    cosine = cosine_table(NT).astype(jnp.float32)
    hartley = hartley_table(NK)
    scale = COUPLING / math.sqrt(NP)
    freq = jnp.einsum('wt,tkpq->wkpq', cosine, chi_time.astype(jnp.float32), precision=highest)
    freq = (scale * freq).astype(jnp.bfloat16)
    screened = lax.map(series_tile, freq.reshape(NT * NK, NP, NP)).reshape(NT, NK, NP, NP)
    timed = jnp.einsum('tw,wkpq->tkpq', cosine, screened.astype(jnp.float32), precision=highest)
    lattice = jnp.einsum('rk,tkpq->rtpq', hartley, timed, precision=highest)
    sigma = (green.astype(jnp.float32) * lattice).astype(jnp.bfloat16)
    coeffs = band_coeffs.astype(jnp.float32)

    def project(tile):
        applied = jnp.dot(tile, band_coeffs, preferred_element_type=jnp.float32)
        return lax.optimization_barrier(jnp.sum(coeffs * applied, axis=0))
    values = lax.map(project, sigma.reshape(NK * NT, NP, NP))
    return values.reshape(NK, NT, NB)
```

```python
import math

import jax
import jax.numpy as jnp
from jax import lax
from jax.sharding import Mesh, PartitionSpec as P

COUPLING = 0.8
JOINT = True


def cosine_table(count):
    index = jnp.arange(count, dtype=jnp.float32) + 0.5
    angle = jnp.pi * index[:, None] * index[None, :] / count
    return (jnp.sqrt(jnp.float32(2.0 / count)) * jnp.cos(angle)).astype(jnp.bfloat16)


def hartley_table(count):
    index = jnp.arange(count, dtype=jnp.float32)
    angle = 2.0 * jnp.pi * index[:, None] * index[None, :] / count
    return (jnp.cos(angle) + jnp.sin(angle)) / jnp.sqrt(jnp.float32(count))


def product(left, right):
    return jnp.einsum("apq,aqs->aps", left, right, preferred_element_type=jnp.float32)


def series(tiles):
    square = product(tiles, tiles).astype(jnp.bfloat16)
    two = (tiles.astype(jnp.float32) + square.astype(jnp.float32)).astype(jnp.bfloat16)
    fourth = product(square, square).astype(jnp.bfloat16)
    four = (two.astype(jnp.float32) + product(two, square)).astype(jnp.bfloat16)
    return (four.astype(jnp.float32) + product(four, fourth)).astype(jnp.bfloat16)


def local(chi_time, green, band_coeffs):
    times_dev, moms_dev, rows_dev, points = chi_time.shape
    momenta, high, low = lax.axis_size("mom"), lax.axis_size("th"), lax.axis_size("tl")
    count_t = times_dev * high * low
    count_k = moms_dev * momenta
    part = rows_dev // low
    piece = part // momenta
    own_k = moms_dev // high
    cosine = cosine_table(count_t)
    hartley = hartley_table(count_k).astype(jnp.bfloat16)
    scale = COUPLING / math.sqrt(points)

    cells_dev = green.shape[0]
    spread = green.reshape(cells_dev, times_dev, low, momenta, piece, points)
    spread = spread.transpose(3, 0, 1, 2, 4, 5)
    spread = lax.all_to_all(spread, "mom", split_axis=0, concat_axis=0, tiled=True)
    spread = spread.reshape(count_k, times_dev, low, piece, points)

    blocks = chi_time.reshape(times_dev, high, own_k, low, part, points)
    blocks = blocks.transpose(1, 3, 0, 2, 4, 5).reshape(high * low, times_dev * own_k, part, points)
    blocks = lax.all_to_all(blocks, ("th", "tl"), split_axis=0, concat_axis=0, tiled=True)
    blocks = blocks.reshape(count_t, own_k, part, points)
    mixed = jnp.einsum("wt,tkpq->wkpq", cosine, blocks, preferred_element_type=jnp.float32)
    mixed = (scale * mixed).astype(jnp.bfloat16).reshape(count_t * own_k, part, points)
    tiles = lax.all_to_all(mixed, ("pt", "tl"), split_axis=0, concat_axis=1, tiled=True)
    screened = series(tiles)
    back = lax.all_to_all(screened, ("pt", "tl"), split_axis=1, concat_axis=0, tiled=True)
    back = back.reshape(count_t, own_k, part, points)
    timed = jnp.einsum("tw,wkpq->tkpq", cosine, back, preferred_element_type=jnp.float32)
    timed = timed.astype(jnp.bfloat16)

    if JOINT:
        timed = timed.reshape(high * low, times_dev, own_k, momenta, piece, points)
        timed = timed.transpose(3, 0, 1, 2, 4, 5)
        timed = timed.reshape(momenta * high * low, times_dev, own_k, piece, points)
        timed = lax.all_to_all(timed, ("mom", "th", "tl"), split_axis=0, concat_axis=0, tiled=True)
    else:
        timed = timed.reshape(high * low, times_dev, own_k, part, points)
        timed = lax.all_to_all(timed, ("th", "tl"), split_axis=0, concat_axis=0, tiled=True)
        timed = timed.reshape(high * low, times_dev, own_k, momenta, piece, points)
        timed = timed.transpose(3, 0, 1, 2, 4, 5)
        timed = lax.all_to_all(timed, "mom", split_axis=0, concat_axis=0, tiled=True)
    timed = timed.reshape(momenta, high, low, times_dev, own_k, piece, points)
    timed = timed.transpose(0, 1, 4, 3, 2, 5, 6).reshape(count_k, times_dev, low, piece, points)
    lattice = jnp.einsum("rk,ktlpq->rtlpq", hartley, timed, preferred_element_type=jnp.float32)
    sigma = (spread.astype(jnp.float32) * lattice).astype(jnp.bfloat16)

    own = lax.dynamic_slice_in_dim(band_coeffs, lax.axis_index("pt") * rows_dev, rows_dev, 0)
    own = own.reshape(low, momenta, piece, -1)
    own = lax.dynamic_index_in_dim(own, lax.axis_index("mom"), 1, keepdims=False)
    applied = jnp.einsum("rtlpq,qn->rtlpn", sigma, band_coeffs, preferred_element_type=jnp.float32)
    partial_sums = jnp.sum(applied * own.astype(jnp.float32)[None, None], axis=(2, 3))
    partial_sums = lax.psum_scatter(partial_sums, "mom", scatter_dimension=0, tiled=True)
    return lax.psum_scatter(partial_sums, "pt", scatter_dimension=2, tiled=True)


def solution(mesh):
    sizes = dict(mesh.shape)
    names, extents = [], []
    for name in mesh.axis_names:
        if name == "tm":
            names += ["th", "tl"]
            extents += [2, sizes[name] // 2]
        else:
            names.append(name)
            extents.append(sizes[name])
    fine = Mesh(mesh.devices.reshape(extents), tuple(names))
    tm = ("th", "tl")
    placed = (P(tm, "mom", "pt", None), P("mom", tm, "pt", None), P())
    return jax.shard_map(
        local, mesh=fine, in_specs=placed, out_specs=P("mom", tm, "pt"), check_vma=False
    )
```
